32 devices in a mesh: expert: 4 (over y, x), tensor: 4 (over z), dp: 2 (over core).
Axes of the slice: x: 2, y: 2, z: 4, core: 2. Of those that a mesh axis runs over, the one named last changes fastest.
Arguments:
- x_real: bfloat16 [2048, 2048], P(('expert', 'dp'), 'tensor'), may hold values from -6 to 6
- routes_real: int32 [2048, 2], P(('expert', 'dp')), may hold values from 0 to 3, all different within a row; in each aligned block of 256 rows (0 to 255, 256 to 511, ...) at most 128 rows name the same one
- gates_real: float32 [2048, 2], P(('expert', 'dp')), may hold values from 0.2 to 1
- up_real: bfloat16 [4, 2048, 8192], P('expert', None, 'tensor'), may hold values from -0.125 to 0.125
- down_real: bfloat16 [4, 8192, 2048], P('expert', 'tensor'), may hold values from -0.0625 to 0.0625
- x_fake: bfloat16 [2048, 2048], P(('expert', 'dp'), 'tensor'), may hold values from -6 to 6
- routes_fake: int32 [2048, 2], P(('expert', 'dp')), may hold values from 0 to 3, all different within a row; in each aligned block of 256 rows (0 to 255, 256 to 511, ...) at most 128 rows name the same one
- gates_fake: float32 [2048, 2], P(('expert', 'dp')), may hold values from 0.2 to 1
- cotangent: bfloat16 [2048, 2048], P(('expert', 'dp'), 'tensor'), may hold values from -6 to 6
- up_fake: bfloat16 [4, 2048, 8192], P('expert', None, 'tensor'), may hold values from -0.125 to 0.125
- down_fake: bfloat16 [4, 8192, 2048], P('expert', 'tensor'), may hold values from -0.0625 to 0.0625
Outputs:
- real_out: bfloat16 [2048, 2048], P(('expert', 'dp'), 'tensor')
- grad_up: bfloat16 [4, 2048, 8192], P('expert', 'dp', 'tensor')
- grad_down: bfloat16 [4, 8192, 2048], P('expert', 'tensor', 'dp')
The draws below stay inside these ranges and needn't reach their ends.
Inputs may be any that keep to these rules, and one draw needn't show every extreme that they name: `routes_real`: each row names 2 different experts. In the 256 rows of one index of expert and dp no expert is named more than 128 times, and that bound is reached. `routes_fake`: each row names 2 different experts. In the 256 rows of one index of expert and dp no expert is named more than 128 times, and that bound is reached.
All inputs are finite; a program needn't handle non-finite values.
Results may differ from the reference program's by a relative error of at most 0.0058.
Values may be sent and summed in bfloat16 or wider, within the bound.
A program may use at most 192 MiB of HBM per device.

```python
import math
import jax
import jax.numpy as jnp
import numpy as np
from jax import lax

D = 2048
FF = 8192
TOP = 2
TOK_DEV = 256
CAP = 128
EXPERTS = 4
TOKENS = 2048


def block_scale(rng, shape, split, smallest, high):
    loudness = 1.0
    for axis_at, blocks in split:
        draws = jax.random.uniform(jax.random.fold_in(jax.random.fold_in(rng, 6), axis_at), (blocks,), jnp.float32, smallest / len(split), high / len(split))
        loudness = loudness * jnp.repeat(jnp.exp(draws), shape[axis_at] // blocks).reshape((-1,) + (1,) * (len(shape) - 1 - axis_at))
    return loudness


def deal_out(stream_key, own, number, rows, count, top, reach, skew):
    order = jax.random.permutation(stream_key, count)
    crowded, usual = load_shares(count, rows * top, reach, skew, True), load_shares(count, rows * top, reach, skew, False)
    places = jnp.arange(count)

    def named(tallies, turn):
        used = int((tallies > 0).sum())
        fixed = max(1, used // 4)
        shifted = fixed + (places - fixed + turn * (used - fixed)) % max(1, count - fixed)
        return jnp.zeros((count,), jnp.int32).at[order[jnp.where(places < fixed, places, shifted)]].set(jnp.asarray(tallies, jnp.int32))

    tallies = jnp.where(number % 4 == 0, named(crowded, number // 4), named(usual, number - number // 4 - 1))
    mixed = jax.random.permutation(jax.random.fold_in(own, 3), count)
    source_of, receiver = mixed[0:count // 2 * 2:2], mixed[1:count // 2 * 2:2]
    margin = jnp.minimum(tallies[source_of] - 1, reach - tallies[receiver]) // 2
    margin = jnp.where((source_of == order[0]) | (receiver == order[0]) | (tallies[receiver] == 0), 0, jnp.maximum(margin, 0))
    shifted = jax.random.randint(jax.random.fold_in(own, 4), (count // 2,), 0, 1 << 20) % (margin + 1)
    tallies = tallies.at[source_of].add(-shifted).at[receiver].add(shifted)
    members = jnp.searchsorted(jnp.cumsum(tallies), jnp.arange(rows * top), side="right").astype(jnp.int32)
    table = members.reshape(top, rows).T
    table = table[jax.random.permutation(jax.random.fold_in(own, 1), rows)]
    turn = jax.random.randint(jax.random.fold_in(own, 2), (rows, 1), 0, top)
    return jnp.take_along_axis(table, (jnp.arange(top)[None, :] + turn) % top, axis=1)


def load_shares(number_of, total, limit, lean, full):
    weights = [(1 << 20) // math.isqrt(rank ** lean) + 1 for rank in range(1, number_of + 1)]
    largest = limit if full else min(limit, max(-(-total // number_of), total * weights[0] // sum(weights)))
    least = 1 if total - largest >= number_of - 1 else 0
    holding, spare = [largest] + [least] * (number_of - 1), total - largest - least * (number_of - 1)
    while spare > 0:
        free = [i for i in range(1, number_of) if holding[i] < largest] or [i for i in range(1, number_of) if holding[i] < limit]
        mass, left = sum([weights[i] for i in free]), spare
        for i in free:
            addition = min(limit - holding[i], max(1, left * weights[i] // mass), spare)
            holding[i] = holding[i] + addition
            spare = spare - addition
    return np.array(holding)


def scatter_about(rng, extent, deviation, bound, shards=(), kind=jnp.bfloat16):
    array = jax.random.normal(rng, extent, jnp.float32) * deviation
    if len(shards) > 0:
        array = block_scale(rng, extent, shards, -0.22, 0.18) * array
    return jnp.clip(array, min=-bound, max=bound).astype(kind)


def setup_inputs(seed: int = 0) -> dict:
    seeds = jax.random.split(jax.random.key(seed), 12)
    x_real = scatter_about(seeds[0], (TOKENS, D), 1.0, 6.0, ((0, 8), (1, 4)))
    routes_real_keys = jax.random.split(jax.random.fold_in(seeds[1], 1), TOKENS // TOK_DEV)
    routes_real_turns = jax.random.permutation(jax.random.fold_in(seeds[1], 3), TOKENS // TOK_DEV)
    routes_real = jax.vmap(lambda own, number: deal_out(jax.random.fold_in(seeds[1], 2), own, number, TOK_DEV, EXPERTS, TOP, CAP, 2))(routes_real_keys, routes_real_turns).reshape((TOKENS, TOP))
    gates_real = jnp.clip(jnp.exp(math.log(1.0) - 1.609438 * jax.random.uniform(seeds[2], (TOKENS, TOP), jnp.float32) ** block_scale(seeds[2], (TOKENS, TOP), ((0, 8),), -0.2, 0.2)), 0.2, 1.0)
    up_real = scatter_about(seeds[3], (EXPERTS, D, FF), D ** -0.5, 0.125, ((0, 4), (2, 4)))
    down_real = scatter_about(seeds[4], (EXPERTS, FF, D), FF ** -0.5, 0.0625, ((0, 4), (1, 4)))
    x_fake = scatter_about(seeds[5], (TOKENS, D), 1.0, 6.0, ((0, 8), (1, 4)))
    routes_fake_keys = jax.random.split(jax.random.fold_in(seeds[6], 1), TOKENS // TOK_DEV)
    routes_fake_turns = jax.random.permutation(jax.random.fold_in(seeds[6], 3), TOKENS // TOK_DEV)
    routes_fake = jax.vmap(lambda own, number: deal_out(jax.random.fold_in(seeds[6], 2), own, number, TOK_DEV, EXPERTS, TOP, CAP, 2))(routes_fake_keys, routes_fake_turns).reshape((TOKENS, TOP))
    gates_fake = jnp.clip(jnp.exp(math.log(1.0) - 1.609438 * jax.random.uniform(seeds[7], (TOKENS, TOP), jnp.float32) ** block_scale(seeds[7], (TOKENS, TOP), ((0, 8),), -0.2, 0.2)), 0.2, 1.0)
    cotangent = scatter_about(seeds[8], (TOKENS, D), 1.0, 6.0, ((0, 8), (1, 4)))
    up_fake = scatter_about(seeds[9], (EXPERTS, D, FF), D ** -0.5, 0.125, ((0, 4), (2, 4)))
    down_fake = scatter_about(seeds[10], (EXPERTS, FF, D), FF ** -0.5, 0.0625, ((0, 4), (1, 4)))
    return dict(x_real=x_real, routes_real=routes_real, gates_real=gates_real, up_real=up_real, down_real=down_real, x_fake=x_fake, routes_fake=routes_fake, gates_fake=gates_fake, cotangent=cotangent, up_fake=up_fake, down_fake=down_fake)


slope_const = 0.7978845608028654
cubic_coef = 0.044715


def gelu_tanh(value):
    return 0.5 * value * (1.0 + jnp.tanh(slope_const * (value + cubic_coef * value * value * value)))


def gelu_slope(value):
    inner = jnp.tanh(slope_const * (value + cubic_coef * value * value * value))
    return 0.5 * (1.0 + inner) + 0.5 * value * (1.0 - inner * inner) * slope_const * (1.0 + 3.0 * cubic_coef * value * value)


def slot_index(routes):
    blocks = routes.reshape(-1, TOK_DEV, TOP)
    labels = jnp.arange(EXPERTS, dtype=jnp.int32)
    hits = (blocks[:, :, :, None] == labels[None, None, None, :]).astype(jnp.int32)
    per_token = jnp.sum(hits, axis=2)
    before = jnp.cumsum(per_token, axis=1) - per_token
    return jnp.sum(hits * before[:, :, None, :], axis=3).reshape(-1, TOP).astype(jnp.int32)


def block_index():
    column = (jnp.arange(TOKENS, dtype=jnp.int32) // TOK_DEV)[:, None]
    return jnp.broadcast_to(column, (TOKENS, TOP)).astype(jnp.int32)


def to_buffer(rows, routes, slots, block):
    count = TOKENS // TOK_DEV
    width = rows.shape[-1]
    buffer = jnp.zeros((EXPERTS, count, CAP, width), rows.dtype)
    return buffer.at[routes, block, slots].set(rows).reshape(EXPERTS, count * CAP, width)


def reference(x_real, routes_real, gates_real, up_real, down_real, x_fake, routes_fake, gates_fake, cotangent, up_fake, down_fake):
    count = TOKENS // TOK_DEV
    block = block_index()
    slots_real = slot_index(routes_real)
    spread_x = jnp.broadcast_to(x_real[:, None, :], (TOKENS, TOP, D))
    buffer_real = to_buffer(spread_x, routes_real, slots_real, block)

    def run_real(item):
        rows, w_up, w_down = item
        hidden = gelu_tanh(jnp.dot(rows, w_up, preferred_element_type=jnp.float32)).astype(jnp.bfloat16)
        return jnp.dot(hidden, w_down, preferred_element_type=jnp.float32).astype(jnp.bfloat16)

    outputs = lax.map(run_real, (buffer_real, up_real, down_real))
    picked = outputs.reshape(EXPERTS, count, CAP, D)[routes_real, block, slots_real]
    real_out = jnp.sum(gates_real[:, :, None] * picked.astype(jnp.float32), axis=1).astype(jnp.bfloat16)

    slots_fake = slot_index(routes_fake)
    scaled = (gates_fake[:, :, None] * cotangent[:, None, :].astype(jnp.float32)).astype(jnp.bfloat16)
    spread_f = jnp.broadcast_to(x_fake[:, None, :], (TOKENS, TOP, D))
    buffer_x = to_buffer(spread_f, routes_fake, slots_fake, block)
    buffer_d = to_buffer(scaled, routes_fake, slots_fake, block)

    def run_fake(item):
        rows_x, rows_d, w_up, w_down = item
        pre = jnp.dot(rows_x, w_up, preferred_element_type=jnp.float32)
        act = gelu_tanh(pre).astype(jnp.bfloat16)
        back = lax.dot_general(rows_d, w_down, (((1,), (1,)), ((), ())), preferred_element_type=jnp.float32)
        dpre = (back * gelu_slope(pre)).astype(jnp.bfloat16)
        grad_in = lax.dot_general(rows_x, dpre, (((0,), (0,)), ((), ())), preferred_element_type=jnp.float32)
        grad_out = lax.dot_general(act, rows_d, (((0,), (0,)), ((), ())), preferred_element_type=jnp.float32)
        return grad_in.astype(jnp.bfloat16), grad_out.astype(jnp.bfloat16)

    grad_up, grad_down = lax.map(run_fake, (buffer_x, buffer_d, up_fake, down_fake))
    return (real_out, grad_up, grad_down)
```

```python
import jax
import jax.numpy as jnp
from jax import lax
from jax.sharding import PartitionSpec as P

slope_const = 0.7978845608028654
cubic_coef = 0.044715


def gelu_tanh(value):
    return (
        0.5 * value * (1.0 + jnp.tanh(slope_const * (value + cubic_coef * value * value * value)))
    )


def gelu_slope(value):
    inner = jnp.tanh(slope_const * (value + cubic_coef * value * value * value))
    return 0.5 * (1.0 + inner) + 0.5 * value * (1.0 - inner * inner) * slope_const * (
        1.0 + 3.0 * cubic_coef * value * value
    )


def slot_index(routes, experts, capacity):
    labels = jnp.arange(experts, dtype=jnp.int32)
    hits = (routes[:, :, None] == labels[None, None, :]).astype(jnp.int32)
    per_token = jnp.sum(hits, axis=1)
    before = jnp.cumsum(per_token, axis=0) - per_token
    slots = jnp.sum(hits * before[:, None, :], axis=2)
    return (routes ^ lax.axis_index("expert")) * capacity + slots


def spread_matrix(position, total):
    rows = jnp.arange(total, dtype=jnp.int32)[:, None]
    match = rows == position[None, :, 0]
    for k in range(1, position.shape[1]):
        match = match | (rows == position[None, :, k])
    return match.astype(jnp.bfloat16)


def slot_gates(position, gates, total):
    rows = jnp.arange(total, dtype=jnp.int32)[:, None]
    picked = jnp.zeros((total, position.shape[0]), jnp.float32)
    for k in range(position.shape[1]):
        picked = jnp.where(rows == position[None, :, k], gates[None, :, k], picked)
    return jnp.sum(picked, axis=1)


def dot32(left, right, dims):
    return lax.dot_general(left, right, (dims, ((), ())), preferred_element_type=jnp.float32)


def hop(value, axis, step):
    return lax.ppermute(value, axis, [(i, i ^ step) for i in range(lax.axis_size(axis))])


def after(value, *others):
    return lax.optimization_barrier((value, *others))[0]


def gather_columns(part, *others):
    size = lax.axis_size("tensor")
    me = lax.axis_index("tensor")
    width = part.shape[1]
    whole = jnp.zeros((part.shape[0], size * width), part.dtype)
    pieces = [hop(part, "tensor", step) for step in range(1, size)]
    pieces = [after(part, *others)] + pieces
    for step, piece in enumerate(pieces):
        whole = lax.dynamic_update_slice(whole, piece, (0, (me ^ step) * width))
    return whole


def exchange(rows, capacity):
    size = lax.axis_size("expert")
    blocks = [rows[:capacity]]
    for step in range(1, size):
        blocks.append(hop(rows[step * capacity : (step + 1) * capacity], "expert", step))
    return jnp.concatenate(blocks, axis=0)


def half_of(rows, step):
    width = rows.shape[1] // lax.axis_size("dp")
    return lax.dynamic_slice_in_dim(rows, (lax.axis_index("dp") ^ step) * width, width, 1)


def on_device(
    x_real,
    routes_real,
    gates_real,
    up_real,
    down_real,
    x_fake,
    routes_fake,
    gates_fake,
    cotangent,
    up_fake,
    down_fake,
):
    experts = lax.axis_size("expert")
    tensors = lax.axis_size("tensor")
    pairs = lax.axis_size("dp")
    tokens, part = x_real.shape
    top = routes_real.shape[1]
    capacity = tokens // 2
    total = experts * capacity

    real_pos = slot_index(routes_real, experts, capacity)
    real_pick = spread_matrix(real_pos, total)
    whole = gather_columns(x_real)
    sent = dot32(real_pick, whole, ((1,), (0,))).astype(jnp.bfloat16)
    rows = exchange(sent, capacity)

    fake_pos = slot_index(routes_fake, experts, capacity)
    fake_pick = spread_matrix(fake_pos, total)
    fake_gate = slot_gates(fake_pos, gates_fake, total)
    whole_x = gather_columns(after(x_fake, real_pos), sent)
    sent_x = dot32(fake_pick, whole_x, ((1,), (0,))).astype(jnp.bfloat16)
    rows_x = exchange(sent_x, capacity)
    whole_c = gather_columns(after(cotangent, whole), sent_x)
    scaled = fake_gate[:, None] * dot32(fake_pick, whole_c, ((1,), (0,)))
    rows_d = exchange(scaled.astype(jnp.bfloat16), capacity)

    hidden = gelu_tanh(dot32(rows, up_real[0], ((1,), (0,)))).astype(jnp.bfloat16)
    partial_out = dot32(hidden, down_real[0], ((1,), (0,))).astype(jnp.bfloat16)
    me = lax.axis_index("tensor")
    mine = [
        lax.dynamic_slice_in_dim(partial_out, (me ^ step) * part, part, 1)
        for step in range(tensors)
    ]
    rows_x = after(rows_x, *mine)
    pre_fake = dot32(rows_x, up_fake[0], ((1,), (0,)))
    act = gelu_tanh(pre_fake).astype(jnp.bfloat16)
    rows_d = after(rows_d, act)
    back_act = dot32(rows_d, down_fake[0], ((1,), (1,)))
    dpre = (back_act * gelu_slope(pre_fake)).astype(jnp.bfloat16)
    grad_in = dot32(half_of(rows_x, 0), dpre, ((0,), (0,)))
    grad_out = dot32(act, half_of(rows_d, 0), ((0,), (0,)))
    summed = after(mine[0], grad_in).astype(jnp.float32)
    for step in range(1, tensors):
        summed = summed + hop(mine[step], "tensor", step).astype(jnp.float32)
    returned = exchange(summed.astype(jnp.bfloat16), capacity)
    columns = jnp.arange(total, dtype=jnp.int32)[None, :]
    real_out = jnp.zeros((tokens, part), jnp.float32)
    for k in range(top):
        pick = (real_pos[:, k][:, None] == columns).astype(jnp.bfloat16)
        real_out = real_out + gates_real[:, k][:, None] * dot32(pick, returned, ((1,), (0,)))
    real_out = real_out.astype(jnp.bfloat16)

    for step in range(1, pairs):
        other_x = hop(half_of(rows_x, step), "dp", step)
        other_act = hop(act, "dp", step)
        other_d = hop(half_of(rows_d, step), "dp", step)
        other_dpre = hop(dpre, "dp", step)
        grad_out = grad_out + dot32(other_act, other_d, ((0,), (0,)))
        grad_in = grad_in + dot32(other_x, other_dpre, ((0,), (0,)))
    return (real_out, grad_in.astype(jnp.bfloat16)[None], grad_out.astype(jnp.bfloat16)[None])


def solution(mesh):
    in_specs = (
        P(("expert", "dp"), "tensor"),
        P(("expert", "dp"), None),
        P(("expert", "dp"), None),
        P("expert", None, "tensor"),
        P("expert", "tensor", None),
        P(("expert", "dp"), "tensor"),
        P(("expert", "dp"), None),
        P(("expert", "dp"), None),
        P(("expert", "dp"), "tensor"),
        P("expert", None, "tensor"),
        P("expert", "tensor", None),
    )
    out_specs = (
        P(("expert", "dp"), "tensor"),
        P("expert", "dp", "tensor"),
        P("expert", "tensor", "dp"),
    )
    return jax.shard_map(
        on_device, mesh=mesh, in_specs=in_specs, out_specs=out_specs, check_vma=False
    )
```
